32 devices in a mesh: pp: 4 (over y, x), cp: 8 (over z, core).
Axes of the slice: x: 2, y: 2, z: 4, core: 2. Of those that a mesh axis runs over, the one named last changes fastest.
Arguments:
- x_in: bfloat16 [4, 1024, 2048], P(None, 'cp'), may hold values from -60 to 80
- norm_gain: float32 [4, 2048], P('pp'), may hold values from 0.5 to 1.5
- w_qkv: bfloat16 [4, 2048, 3072], P('pp', 'cp'), may hold values from -0.13258252 to 1.307771
- w_out: bfloat16 [4, 2048, 2048], P('pp', 'cp'), may hold values from -0.125 to 0.125
- cycle_size: int32 [4], replicated, may hold values from 2 to 8, as said below
- token_pos: int32 [4, 1024], replicated, may hold values from 0 to 1023, as said below
- doc_starts: int32 [4, 16], replicated, may hold values from 0 to 1024, as said below
Outputs:
- layer_outputs: bfloat16 [4, 4, 1024, 2048], P('pp', None, 'cp')
The draws below stay inside these ranges and needn't reach their ends.
Inputs may be any that keep to these rules, and one draw needn't show every extreme that they name: `cycle_size`: powers of two dividing the devices of cp; some micro-batch has 8 and some has 2. `token_pos`: for a micro-batch with group size r, every aligned block of r * 128 slots holds each position of that block once. `doc_starts`: for a micro-batch with group size r and g below 8 / r, entry 2 g is g * r * 128 and entry 2 g + 1 either lies strictly inside that group's positions or is 1024, so each group holds one or two documents; the remaining entries are 1024.
All inputs are finite; a program needn't handle non-finite values.
Results may differ from the reference program's by a relative error of at most 0.0075.
Values may be sent and summed in bfloat16 or wider, within the bound.
No kernel may reach another device: no remote copies, remote signals or barrier semaphores. Data moves between devices by JAX's collectives and lax.ppermute only.
A program may use at most 128 MiB of HBM per device.

```python
import math
import jax
import jax.numpy as jnp
from jax import lax

D = 2048
HEADS = 16
KV_HEADS = 4
HEAD_DIM = 128
T_DEV = 128
MICRO = 4
CYCLE_MAX = 8
LAYERS = 4
TOKENS = 1024
DOCS = 16
QKV_COLS = 3072


def cycle_draw(key):
    levels = CYCLE_MAX.bit_length() - 1
    exponent = jax.random.randint(key, (MICRO,), 1, levels + 1).astype(jnp.int32)
    sizes_drawn = jnp.left_shift(jnp.int32(1), exponent)
    chosen = jax.random.randint(jax.random.fold_in(key, 1), (), 0, MICRO)
    other = (chosen + jax.random.randint(jax.random.fold_in(key, 2), (), 1, MICRO)) % MICRO
    index = jnp.arange(MICRO)
    sizes_drawn = jnp.where(index == other, 2, sizes_drawn)
    return jnp.where(index == chosen, CYCLE_MAX, sizes_drawn).astype(jnp.int32)


def draw_cycle_size(key, part):
    return cycle_draw(jax.random.fold_in(key, 11))


def draw_token_pos(key, part):
    cycles = cycle_draw(jax.random.fold_in(key, 11))

    def one_row(row_key, cycle_devices):
        span = cycle_devices * T_DEV
        slots = jnp.arange(TOKENS, dtype=jnp.int32)
        groups = slots // span
        noise = jax.random.permutation(row_key, TOKENS).astype(jnp.int32)
        ordered = jnp.argsort(groups * TOKENS + noise, stable=True)
        return jnp.zeros((TOKENS,), jnp.int32).at[ordered].set(slots)
    row_keys = jax.random.split(jax.random.fold_in(key, 12), MICRO)
    return jax.vmap(one_row)(row_keys, cycles)


def draw_doc_starts(key, part):
    cycles = cycle_draw(jax.random.fold_in(key, 11))
    group_slots = DOCS // 2

    def one_row(row_key, cycle_devices):
        span = cycle_devices * T_DEV
        live_groups = group_slots // cycle_devices
        index = jnp.arange(group_slots, dtype=jnp.int32)
        inside = jax.random.randint(row_key, (group_slots,), 1, span).astype(jnp.int32)
        split_here = jax.random.randint(jax.random.fold_in(row_key, 5), (group_slots,), 0, 2) == 1
        first_pos = index * span
        second_pos = jnp.where(split_here, first_pos + inside, TOKENS)
        paired = jnp.stack([first_pos, second_pos], axis=1).reshape(-1)
        live = jnp.repeat(index < live_groups, 2)
        return jnp.where(live, paired, TOKENS).astype(jnp.int32)
    row_keys = jax.random.split(jax.random.fold_in(key, 13), MICRO)
    return jax.vmap(one_row)(row_keys, cycles)


def draw_x_in(key, part):
    base_draw = jnp.clip(jax.random.normal(jax.random.fold_in(key, 21), (MICRO, TOKENS, D), jnp.float32), -6.0, 6.0)
    return base_draw.astype(jnp.bfloat16)


def draw_w_qkv(key, part):
    base_draw = jnp.clip(jax.random.normal(jax.random.fold_in(key, 31), (LAYERS, D, QKV_COLS), jnp.float32), -6.0, 6.0) * D ** (-0.5)
    return base_draw.astype(jnp.bfloat16)


def block_levels(rng, extent, shards, smallest, top_value):
    def one(position, blocks):
        draws = jax.random.uniform(jax.random.fold_in(jax.random.fold_in(rng, 6), position), (blocks,), jnp.float32, smallest / len(shards), top_value / len(shards))
        return jnp.repeat(jnp.exp(draws), extent[position] // blocks).reshape((-1,) + (1,) * (len(extent) - position - 1))

    gain = one(*shards[0])
    for cut in shards[1:]:
        gain = gain * one(*cut)
    return gain


def centred(stream_key, extent, width, bound, cuts=(), held_as=jnp.bfloat16):
    gain = block_levels(stream_key, extent, cuts, -0.22, 0.18) if cuts else 1.0
    array = jax.random.normal(stream_key, extent, jnp.float32) * width * gain
    return jnp.minimum(jnp.maximum(array, -bound), bound).astype(held_as)


def setup_inputs(seed: int = 0) -> dict:
    seeds = jax.random.split(jax.random.key(seed), 8)
    return {
        "x_in": draw_x_in(jax.random.fold_in(seeds[7], 71), 0),
        "norm_gain": jnp.clip(1.0 + 0.1 * jax.random.normal(seeds[1], (LAYERS, D), jnp.float32), 0.5, 1.5),
        "w_qkv": draw_w_qkv(jax.random.fold_in(seeds[7], 71), 0),
        "w_out": centred(seeds[3], (LAYERS, HEADS * HEAD_DIM, D), (HEADS * HEAD_DIM) ** -0.5, 0.125, ((0, 4), (1, 8))),
        "cycle_size": draw_cycle_size(jax.random.fold_in(seeds[7], 71), 0),
        "token_pos": draw_token_pos(jax.random.fold_in(seeds[7], 71), 0),
        "doc_starts": draw_doc_starts(jax.random.fold_in(seeds[7], 71), 0),
    }


epsilon = 1e-05
rope_base = 500000.0

def rotate(values, relative):
    half_dim = values.shape[-1] // 2
    frequency_index = jnp.arange(half_dim, dtype=jnp.float32)
    inverse = jnp.power(jnp.float32(rope_base), -2.0 * frequency_index / values.shape[-1])
    angles = relative.astype(jnp.float32)[:, None] * inverse[None, :]
    cosine = jnp.cos(angles)[:, None, :]
    sine_part = jnp.sin(angles)[:, None, :]
    first_half = values[..., :half_dim]
    second_half = values[..., half_dim:]
    return jnp.concatenate([first_half * cosine - second_half * sine_part, second_half * cosine + first_half * sine_part], axis=-1)

def doc_begin(positions, starts):
    at_or_below = starts[None, :] <= positions[:, None]
    return lax.optimization_barrier(jnp.max(jnp.where(at_or_below, starts[None, :], 0), axis=1)).astype(jnp.int32)

def layer_forward(hidden, gain_row, qkv_weight, out_weight, positions, starts, cycle_devices):
    widened = hidden.astype(jnp.float32)
    mean_square = lax.optimization_barrier(jnp.mean(widened * widened, axis=-1, keepdims=True))
    normed = (widened * lax.rsqrt(mean_square + epsilon) * gain_row.astype(jnp.float32)).astype(jnp.bfloat16)
    projected = jnp.dot(normed, qkv_weight, preferred_element_type=jnp.float32)
    query_cols = HEADS * HEAD_DIM
    key_cols = KV_HEADS * HEAD_DIM
    begins = doc_begin(positions, starts)
    relative = positions - begins
    queries = rotate(projected[:, :query_cols].reshape(-1, HEADS, HEAD_DIM), relative).astype(jnp.bfloat16)
    keys_all = rotate(projected[:, query_cols:query_cols + key_cols].reshape(-1, KV_HEADS, HEAD_DIM), relative).astype(jnp.bfloat16)
    values_all = projected[:, query_cols + key_cols:].reshape(-1, KV_HEADS, HEAD_DIM).astype(jnp.bfloat16)
    groups = positions // (cycle_devices * T_DEV)
    window = CYCLE_MAX * T_DEV
    block_rows = math.gcd(window, 512)
    block_count = TOKENS // block_rows

    def attend(pieces):
        block_queries, block_pos, block_begin, block_group, block_number = pieces
        window_start = (block_number * block_rows // window * window).astype(jnp.int32)
        near_keys = lax.dynamic_slice_in_dim(keys_all, window_start, window, 0)
        near_values = lax.dynamic_slice_in_dim(values_all, window_start, window, 0)
        near_pos = lax.dynamic_slice_in_dim(positions, window_start, window, 0)
        near_begin = lax.dynamic_slice_in_dim(begins, window_start, window, 0)
        near_group = lax.dynamic_slice_in_dim(groups, window_start, window, 0)
        grouped = block_queries.astype(jnp.float32).reshape(block_rows, KV_HEADS, HEADS // KV_HEADS, HEAD_DIM)
        scores = jnp.einsum('bkgd,skd->kgbs', grouped, near_keys.astype(jnp.float32)) * HEAD_DIM ** (-0.5)
        visible = (block_group[:, None] == near_group[None, :]) & (block_begin[:, None] == near_begin[None, :]) & (near_pos[None, :] <= block_pos[:, None])
        scores = jnp.where(visible[None, None], scores, -1e+30)
        row_max = lax.optimization_barrier(jnp.max(scores, axis=-1, keepdims=True))
        weights_exp = jnp.exp(scores - row_max)
        row_sum = lax.optimization_barrier(jnp.sum(weights_exp, axis=-1, keepdims=True))
        rounded = lax.optimization_barrier(weights_exp.astype(jnp.bfloat16)).astype(jnp.float32)
        combined = jnp.einsum('kgbs,skd->kgbd', rounded, near_values.astype(jnp.float32)) / row_sum
        return jnp.transpose(combined, (2, 0, 1, 3)).reshape(block_rows, query_cols).astype(jnp.bfloat16)
    attended = lax.map(attend, (queries.reshape(block_count, block_rows, HEADS, HEAD_DIM), positions.reshape(block_count, block_rows), begins.reshape(block_count, block_rows), groups.reshape(block_count, block_rows), jnp.arange(block_count, dtype=jnp.int32)))
    attended = attended.reshape(TOKENS, query_cols)
    output = jnp.dot(attended, out_weight, preferred_element_type=jnp.float32)
    return (widened + output).astype(jnp.bfloat16)

def reference(x_in, norm_gain, w_qkv, w_out, cycle_size, token_pos, doc_starts):
    per_micro = []
    for micro_index in range(MICRO):
        hidden = x_in[micro_index]
        layer_rows = []
        for layer_index in range(LAYERS):
            hidden = layer_forward(hidden, norm_gain[layer_index], w_qkv[layer_index], w_out[layer_index], token_pos[micro_index], doc_starts[micro_index], cycle_size[micro_index])
            layer_rows.append(hidden)
        per_micro.append(jnp.stack(layer_rows))
    return jnp.stack(per_micro, axis=1)
```

```python
import functools
import math

import jax
import jax.numpy as jnp
from jax import lax
from jax.experimental import pallas as pl
from jax.experimental.pallas import tpu as pltpu
from jax.sharding import PartitionSpec as P

HEADS = 16
KV_HEADS = 4
HEAD_DIM = 128
CYCLE_MAX = 8
GROUP = HEADS // KV_HEADS
QUERY_COLS = HEADS * HEAD_DIM
KEY_COLS = KV_HEADS * HEAD_DIM

epsilon = 1e-05
rope_base = 500000.0


def swapped(array, bit):
    return lax.ppermute(array, "cp", [(i, i ^ 1 << bit) for i in range(lax.axis_size("cp"))])


def rotate_heads(values, cosine, sine):
    heads = []
    for h in range(values.shape[-1] // HEAD_DIM):
        head = values[:, h * HEAD_DIM : (h + 1) * HEAD_DIM]
        heads.append(head * cosine + pltpu.roll(head, HEAD_DIM // 2, 1) * sine)
    return jnp.concatenate(heads, axis=1)


def kv_kernel(mi_ref, hidden_ref, gain_ref, w_ref, cos_ref, sin_ref, key_ref, value_ref, normed_ref):
    step = pl.program_id(0)

    @pl.when(step == 0)
    def _():
        widened = hidden_ref[...].astype(jnp.float32)
        mean_square = jnp.mean(widened * widened, axis=-1, keepdims=True)
        normed_ref[...] = (widened * lax.rsqrt(mean_square + epsilon) * gain_ref[...]).astype(jnp.bfloat16)

    projected = jnp.dot(normed_ref[...], w_ref[...], preferred_element_type=jnp.float32)

    @pl.when(step == 0)
    def _():
        key_ref[...] = rotate_heads(projected, cos_ref[0], sin_ref[0]).astype(jnp.bfloat16)

    @pl.when(step == 1)
    def _():
        value_ref[...] = projected.astype(jnp.bfloat16)


def query_kernel(mi_ref, normed_ref, w_ref, cos_ref, sin_ref, query_ref):
    projected = jnp.dot(normed_ref[...], w_ref[...], preferred_element_type=jnp.float32)
    query_ref[...] = rotate_heads(projected, cos_ref[0], sin_ref[0]).astype(jnp.bfloat16)


def back_kernel(
    mi_ref, query_ref, *refs
):
    count = (len(refs) - 9) // 2
    key_refs, value_refs = refs[:count], refs[count : 2 * count]
    qcode_ref, qpos_ref, kcode_ref, kpos_ref, hidden_ref, w_ref, out_ref, acc_ref, bias_ref = refs[2 * count :]
    step = pl.program_id(0)

    @pl.when(step == 0)
    def _():
        visible = (qcode_ref[0] == kcode_ref[0]) & (kpos_ref[0] <= qpos_ref[0])
        bias_ref[...] = jnp.where(visible, 0.0, -1e30).astype(jnp.float32)
        acc_ref[...] = hidden_ref[...].astype(jnp.float32)

    part = key_refs[0].shape[0]
    factor = HEAD_DIM ** (-0.5) * math.log2(math.e)
    heads = []
    for g in range(GROUP):
        query = query_ref[:, g * HEAD_DIM : (g + 1) * HEAD_DIM]
        scores = [
            lax.dot_general(query, ref[...], (((1,), (1,)), ((), ())), preferred_element_type=jnp.float32)
            + bias_ref[:, i * part : (i + 1) * part]
            for i, ref in enumerate(key_refs)
        ]
        row_max = functools.reduce(jnp.maximum, [jnp.max(s, axis=-1, keepdims=True) for s in scores])
        exps = [jnp.exp2((s - row_max) * factor) for s in scores]
        row_sum = sum(jnp.sum(e, axis=-1, keepdims=True) for e in exps)
        combined = sum(
            jnp.dot(e.astype(jnp.bfloat16), ref[...], preferred_element_type=jnp.float32)
            for e, ref in zip(exps, value_refs)
        )
        heads.append((combined / row_sum).astype(jnp.bfloat16))
    attended = jnp.concatenate(heads, axis=1)
    acc_ref[...] += jnp.dot(attended, w_ref[...], preferred_element_type=jnp.float32)

    @pl.when(step == KV_HEADS - 1)
    def _():
        out_ref[...] = acc_ref[...].astype(jnp.bfloat16)


def call(kernel, grid, in_specs, out_specs, out_shape, scratch=(), name=None):
    return pl.pallas_call(
        kernel,
        grid_spec=pltpu.PrefetchScalarGridSpec(
            num_scalar_prefetch=1,
            grid=(grid,),
            in_specs=in_specs,
            out_specs=out_specs,
            scratch_shapes=scratch,
        ),
        out_shape=out_shape,
        name=name,
    )


def whole_spec(shape):
    return pl.BlockSpec(shape, lambda j, mi: (0,) * len(shape))


def micro_spec(shape):
    return pl.BlockSpec((1,) + shape, lambda j, mi: (mi[0],) + (0,) * len(shape))


def project_kv(mi, hidden, gain, weight, cosine, sine):
    rows, width = hidden.shape
    first = QUERY_COLS // KEY_COLS
    return call(
        kv_kernel,
        2,
        [
            whole_spec((rows, width)),
            whole_spec((1, width)),
            pl.BlockSpec((width, KEY_COLS), lambda j, mi: (0, first + j)),
            micro_spec((rows, HEAD_DIM)),
            micro_spec((rows, HEAD_DIM)),
        ],
        [whole_spec((rows, KEY_COLS)), whole_spec((rows, KEY_COLS)), whole_spec((rows, width))],
        [
            jax.ShapeDtypeStruct((rows, KEY_COLS), jnp.bfloat16),
            jax.ShapeDtypeStruct((rows, KEY_COLS), jnp.bfloat16),
            jax.ShapeDtypeStruct((rows, width), jnp.bfloat16),
        ],
        name="project_kv",
    )(mi, hidden, gain, weight, cosine, sine)


def project_query(mi, normed, weight, cosine, sine):
    rows, width = normed.shape
    cols = QUERY_COLS // 4
    return call(
        query_kernel,
        4,
        [
            whole_spec((rows, width)),
            pl.BlockSpec((width, cols), lambda j, mi: (0, j)),
            micro_spec((rows, HEAD_DIM)),
            micro_spec((rows, HEAD_DIM)),
        ],
        pl.BlockSpec((rows, cols), lambda j, mi: (0, j)),
        jax.ShapeDtypeStruct((rows, QUERY_COLS), jnp.bfloat16),
        name="project_query",
    )(mi, normed, weight, cosine, sine)


def attend_out(mi, query, keys, values, tables, hidden, weight):
    rows, width = hidden.shape
    cols = GROUP * HEAD_DIM
    key_rows = sum(k.shape[0] for k in keys)
    kv_specs = [pl.BlockSpec((k.shape[0], HEAD_DIM), lambda j, mi: (0, j)) for k in keys]
    return call(
        back_kernel,
        KV_HEADS,
        [pl.BlockSpec((rows, cols), lambda j, mi: (0, j))]
        + kv_specs
        + kv_specs
        + [
            micro_spec((rows, 1)),
            micro_spec((rows, 1)),
            micro_spec((1, key_rows)),
            micro_spec((1, key_rows)),
            whole_spec((rows, width)),
            pl.BlockSpec((cols, width), lambda j, mi: (j, 0)),
        ],
        whole_spec((rows, width)),
        jax.ShapeDtypeStruct((rows, width), jnp.bfloat16),
        scratch=[pltpu.VMEM((rows, width), jnp.float32), pltpu.VMEM((rows, key_rows), jnp.float32)],
        name="attend_out",
    )(mi, query, *keys, *values, *tables, hidden, weight)


def collect(own):
    block = own
    for bit in reversed(range(1, CYCLE_MAX.bit_length() - 1)):
        block = jnp.concatenate([block, swapped(block, bit)], axis=0)
    return [block, swapped(block, 0)]


def key_order():
    order = [0]
    for bit in reversed(range(CYCLE_MAX.bit_length() - 1)):
        order = order + [b ^ 1 << bit for b in order]
    return order


def body(x_in, norm_gain, w_qkv, w_out, cycle_size, token_pos, doc_starts):
    sections = lax.axis_size("pp")
    section_index = lax.axis_index("pp")
    device = lax.axis_index("cp")
    micro_count, tok_rows, model_width = x_in.shape
    tokens = token_pos.shape[1]

    begins = jnp.max(
        jnp.where(doc_starts[:, None, :] <= token_pos[:, :, None], doc_starts[:, None, :], 0), axis=2
    )
    codes = token_pos // (cycle_size * tok_rows)[:, None] * tokens + begins
    by_device = lambda a: a.reshape(micro_count, tokens // tok_rows, tok_rows)
    pos_blocks, begin_blocks, code_blocks = by_device(token_pos), by_device(begins), by_device(codes)
    take = lambda a, b: lax.dynamic_index_in_dim(a, device ^ b, 1, keepdims=False)
    own_pos, own_begin, own_code = take(pos_blocks, 0), take(begin_blocks, 0), take(code_blocks, 0)
    order = key_order()
    key_pos = jnp.concatenate([take(pos_blocks, b) for b in order], axis=1)[:, None, :]
    key_code = jnp.concatenate([take(code_blocks, b) for b in order], axis=1)[:, None, :]
    tables = (own_code[:, :, None], own_pos[:, :, None], key_code, key_pos)
    half_dim = HEAD_DIM // 2
    inverse = jnp.power(
        jnp.float32(rope_base), -2.0 * jnp.arange(half_dim, dtype=jnp.float32) / HEAD_DIM
    )
    angles = (own_pos - own_begin).astype(jnp.float32)[:, :, None] * inverse
    cos_half, sin_half = jnp.cos(angles), jnp.sin(angles)
    cosine = jnp.concatenate([cos_half, cos_half], axis=-1)
    sine = jnp.concatenate([-sin_half, sin_half], axis=-1)

    qkv_full = lax.all_gather(w_qkv, "cp", axis=1, tiled=True)[0]
    out_full = lax.all_gather(w_out, "cp", axis=1, tiled=True)[0]

    outputs = jnp.zeros((micro_count, tok_rows, model_width), jnp.bfloat16)
    carried = None
    turn_count = micro_count + sections - 1
    for turn in range(turn_count):
        offset = turn - section_index
        micro_index = jnp.clip(offset, 0, micro_count - 1)
        mi = micro_index.astype(jnp.int32).reshape(1)
        if turn == 0:
            hidden = x_in[0]
        elif turn < micro_count:
            hidden = jnp.where(section_index == 0, x_in[turn], carried)
        else:
            hidden = carried
        key_own, value_own, normed = project_kv(mi, hidden, norm_gain, qkv_full, cosine, sine)
        keys, values = collect(key_own), collect(value_own)
        query = project_query(mi, normed, qkv_full, cosine, sine)
        result = attend_out(mi, query, keys, values, tables, hidden, out_full)
        if turn + 1 < turn_count:
            carried = lax.ppermute(result, "pp", [(i, i + 1) for i in range(sections - 1)])
        kept = result
        if turn >= micro_count:
            kept = jnp.where(offset < micro_count, result, outputs[micro_count - 1])
        outputs = lax.dynamic_update_index_in_dim(outputs, kept, micro_index, 0)
    return outputs[None]


def solution(mesh):
    in_specs = (
        P(None, "cp", None),
        P("pp", None),
        P("pp", "cp", None),
        P("pp", "cp", None),
        P(),
        P(),
        P(),
    )
    out_specs = P("pp", None, "cp", None)
    return jax.shard_map(body, mesh=mesh, in_specs=in_specs, out_specs=out_specs, check_vma=False)
```

```python
import functools
import math

import jax
import jax.numpy as jnp
from jax import lax
from jax.experimental import pallas as pl
from jax.experimental.pallas import tpu as pltpu
from jax.sharding import PartitionSpec as P

HEADS = 16
KV_HEADS = 4
HEAD_DIM = 128
CYCLE_MAX = 8
GROUP = HEADS // KV_HEADS
QUERY_COLS = HEADS * HEAD_DIM
KEY_COLS = KV_HEADS * HEAD_DIM

epsilon = 1e-05
rope_base = 500000.0


def swapped(array, bit):
    return lax.ppermute(array, "cp", [(i, i ^ 1 << bit) for i in range(lax.axis_size("cp"))])


def rotate_heads(values, cosine, sine):
    heads = []
    for h in range(values.shape[-1] // HEAD_DIM):
        head = values[:, h * HEAD_DIM : (h + 1) * HEAD_DIM]
        heads.append(head * cosine + pltpu.roll(head, HEAD_DIM // 2, 1) * sine)
    return jnp.concatenate(heads, axis=1)


def kv_kernel(mi_ref, hidden_ref, gain_ref, w_ref, cos_ref, sin_ref, piece_ref, normed_ref):
    step = pl.program_id(0)
    rows = cos_ref.shape[1]

    @pl.when(step == 0)
    def _():
        widened = hidden_ref[...].astype(jnp.float32)
        mean_square = jnp.mean(widened * widened, axis=-1, keepdims=True)
        normed_ref[...] = (widened * lax.rsqrt(mean_square + epsilon) * gain_ref[...]).astype(jnp.bfloat16)

    projected = jnp.dot(normed_ref[...], w_ref[...], preferred_element_type=jnp.float32)

    @pl.when(step == 0)
    def _():
        piece_ref[:rows, :] = rotate_heads(projected, cos_ref[0], sin_ref[0]).astype(jnp.bfloat16)

    @pl.when(step == 1)
    def _():
        piece_ref[rows:, :] = projected.astype(jnp.bfloat16)


def query_kernel(mi_ref, normed_ref, w_ref, cos_ref, sin_ref, query_ref):
    projected = jnp.dot(normed_ref[...], w_ref[...], preferred_element_type=jnp.float32)
    query_ref[...] = rotate_heads(projected, cos_ref[0], sin_ref[0]).astype(jnp.bfloat16)


def back_kernel(mi_ref, query_ref, *refs):
    piece_refs = refs[:-9]
    qcode_ref, qpos_ref, kcode_ref, kpos_ref, hidden_ref, w_ref, out_ref, acc_ref, bias_ref = refs[-9:]
    step = pl.program_id(0)

    @pl.when(step == 0)
    def _():
        visible = (qcode_ref[0] == kcode_ref[0]) & (kpos_ref[0] <= qpos_ref[0])
        bias_ref[...] = jnp.where(visible, 0.0, -1e30).astype(jnp.float32)
        acc_ref[...] = hidden_ref[...].astype(jnp.float32)

    rows = query_ref.shape[0]
    part = piece_refs[0].shape[0] // 2
    factor = HEAD_DIM ** (-0.5) * math.log2(math.e)
    query = jnp.concatenate([query_ref[:, g * HEAD_DIM : (g + 1) * HEAD_DIM] for g in range(GROUP)], axis=0)
    scores = [
        lax.dot_general(query, ref[:part, :], (((1,), (1,)), ((), ())), preferred_element_type=jnp.float32)
        + jnp.concatenate([bias_ref[:, i * part : (i + 1) * part]] * GROUP, axis=0)
        for i, ref in enumerate(piece_refs)
    ]
    row_max = jnp.max(functools.reduce(jnp.maximum, scores), axis=-1, keepdims=True)
    exps = [jnp.exp2((s - row_max) * factor) for s in scores]
    row_sum = jnp.sum(functools.reduce(jnp.add, exps), axis=-1, keepdims=True)
    combined = functools.reduce(
        jnp.add,
        [
            jnp.dot(e.astype(jnp.bfloat16), ref[part:, :], preferred_element_type=jnp.float32)
            for e, ref in zip(exps, piece_refs)
        ],
    )
    heads = (combined / row_sum).astype(jnp.bfloat16)
    attended = jnp.concatenate([heads[g * rows : (g + 1) * rows] for g in range(GROUP)], axis=1)
    acc_ref[...] += jnp.dot(attended, w_ref[...], preferred_element_type=jnp.float32)

    @pl.when(step == KV_HEADS - 1)
    def _():
        out_ref[...] = acc_ref[...].astype(jnp.bfloat16)


def call(kernel, grid, in_specs, out_specs, out_shape, scratch=(), name=None):
    return pl.pallas_call(
        kernel,
        grid_spec=pltpu.PrefetchScalarGridSpec(
            num_scalar_prefetch=1,
            grid=(grid,),
            in_specs=in_specs,
            out_specs=out_specs,
            scratch_shapes=scratch,
        ),
        out_shape=out_shape,
        name=name,
    )


def whole_spec(shape):
    return pl.BlockSpec(shape, lambda j, mi: (0,) * len(shape))


def micro_spec(shape):
    return pl.BlockSpec((1,) + shape, lambda j, mi: (mi[0],) + (0,) * len(shape))


def project_kv(mi, hidden, gain, weight, cosine, sine):
    rows, width = hidden.shape
    first = QUERY_COLS // KEY_COLS
    return call(
        kv_kernel,
        2,
        [
            whole_spec((rows, width)),
            whole_spec((1, width)),
            pl.BlockSpec((width, KEY_COLS), lambda j, mi: (0, first + j)),
            micro_spec((rows, HEAD_DIM)),
            micro_spec((rows, HEAD_DIM)),
        ],
        [whole_spec((2 * rows, KEY_COLS)), whole_spec((rows, width))],
        [
            jax.ShapeDtypeStruct((2 * rows, KEY_COLS), jnp.bfloat16),
            jax.ShapeDtypeStruct((rows, width), jnp.bfloat16),
        ],
        name="project_kv",
    )(mi, hidden, gain, weight, cosine, sine)


def project_query(mi, normed, weight, cosine, sine):
    rows, width = normed.shape
    cols = QUERY_COLS // 4
    return call(
        query_kernel,
        4,
        [
            whole_spec((rows, width)),
            pl.BlockSpec((width, cols), lambda j, mi: (0, j)),
            micro_spec((rows, HEAD_DIM)),
            micro_spec((rows, HEAD_DIM)),
        ],
        pl.BlockSpec((rows, cols), lambda j, mi: (0, j)),
        jax.ShapeDtypeStruct((rows, QUERY_COLS), jnp.bfloat16),
        name="project_query",
    )(mi, normed, weight, cosine, sine)


def attend_out(mi, query, pieces, tables, hidden, weight):
    rows, width = hidden.shape
    cols = GROUP * HEAD_DIM
    key_rows = sum(p.shape[0] for p in pieces) // 2
    return call(
        back_kernel,
        KV_HEADS,
        [pl.BlockSpec((rows, cols), lambda j, mi: (0, j))]
        + [pl.BlockSpec((p.shape[0], HEAD_DIM), lambda j, mi: (0, j)) for p in pieces]
        + [
            micro_spec((rows, 1)),
            micro_spec((rows, 1)),
            micro_spec((1, key_rows)),
            micro_spec((1, key_rows)),
            whole_spec((rows, width)),
            pl.BlockSpec((cols, width), lambda j, mi: (j, 0)),
        ],
        whole_spec((rows, width)),
        jax.ShapeDtypeStruct((rows, width), jnp.bfloat16),
        scratch=[pltpu.VMEM((rows, width), jnp.float32), pltpu.VMEM((rows, key_rows), jnp.float32)],
        name="attend_out",
    )(mi, query, *pieces, *tables, hidden, weight)


def collect(own, make_query):
    pieces = [own]
    query = None
    for bit in reversed(range(CYCLE_MAX.bit_length() - 1)):
        arrived = [swapped(piece, bit) for piece in pieces]
        if query is None:
            query = make_query()
            arrived[0], query = lax.optimization_barrier((arrived[0], query))
        pieces = pieces + arrived
    return pieces, query


def key_order():
    order = [0]
    for bit in reversed(range(CYCLE_MAX.bit_length() - 1)):
        order = order + [b ^ 1 << bit for b in order]
    return order


def body(x_in, norm_gain, w_qkv, w_out, cycle_size, token_pos, doc_starts):
    sections = lax.axis_size("pp")
    section_index = lax.axis_index("pp")
    device = lax.axis_index("cp")
    micro_count, tok_rows, model_width = x_in.shape
    tokens = token_pos.shape[1]

    begins = jnp.max(
        jnp.where(doc_starts[:, None, :] <= token_pos[:, :, None], doc_starts[:, None, :], 0), axis=2
    )
    codes = token_pos // (cycle_size * tok_rows)[:, None] * tokens + begins
    by_device = lambda a: a.reshape(micro_count, tokens // tok_rows, tok_rows)
    pos_blocks, begin_blocks, code_blocks = by_device(token_pos), by_device(begins), by_device(codes)
    take = lambda a, b: lax.dynamic_index_in_dim(a, device ^ b, 1, keepdims=False)
    own_pos, own_begin, own_code = take(pos_blocks, 0), take(begin_blocks, 0), take(code_blocks, 0)
    order = key_order()
    key_pos = jnp.concatenate([take(pos_blocks, b) for b in order], axis=1)[:, None, :]
    key_code = jnp.concatenate([take(code_blocks, b) for b in order], axis=1)[:, None, :]
    tables = (own_code[:, :, None], own_pos[:, :, None], key_code, key_pos)
    half_dim = HEAD_DIM // 2
    inverse = jnp.power(
        jnp.float32(rope_base), -2.0 * jnp.arange(half_dim, dtype=jnp.float32) / HEAD_DIM
    )
    angles = (own_pos - own_begin).astype(jnp.float32)[:, :, None] * inverse
    cos_half, sin_half = jnp.cos(angles), jnp.sin(angles)
    cosine = jnp.concatenate([cos_half, cos_half], axis=-1)
    sine = jnp.concatenate([-sin_half, sin_half], axis=-1)

    qkv_full = lax.all_gather(w_qkv, "cp", axis=1, tiled=True)[0]
    out_full = lax.all_gather(w_out, "cp", axis=1, tiled=True)[0]

    outputs = jnp.zeros((micro_count, tok_rows, model_width), jnp.bfloat16)
    carried = None
    ahead = [(i, i + 1) for i in range(sections - 1)]
    turn_count = micro_count + sections - 1
    for turn in range(turn_count):
        offset = turn - section_index
        micro_index = jnp.clip(offset, 0, micro_count - 1)
        mi = micro_index.astype(jnp.int32).reshape(1)
        if turn == 0:
            hidden = x_in[0]
        elif turn < micro_count:
            hidden = jnp.where(section_index == 0, x_in[turn], carried)
        else:
            hidden = carried
        own, normed = project_kv(mi, hidden, norm_gain, qkv_full, cosine, sine)
        pieces, query = collect(own, lambda: project_query(mi, normed, qkv_full, cosine, sine))
        result = attend_out(mi, query, pieces, tables, hidden, out_full)
        if turn + 1 < turn_count:
            carried = lax.ppermute(result, "pp", ahead)
        kept = result
        if turn >= micro_count:
            kept = jnp.where(offset < micro_count, result, outputs[micro_count - 1])
        outputs = lax.dynamic_update_index_in_dim(outputs, kept, micro_index, 0)
    return outputs[None]


def solution(mesh):
    in_specs = (
        P(None, "cp", None),
        P("pp", None),
        P("pp", "cp", None),
        P("pp", "cp", None),
        P(),
        P(),
        P(),
    )
    out_specs = P("pp", None, "cp", None)
    return jax.shard_map(body, mesh=mesh, in_specs=in_specs, out_specs=out_specs, check_vma=False)
```
